16 devices in a mesh: rep: 1, r: 2 (over z), s: 8 (over x, y, core).
Axes of the slice: x: 2, y: 2, z: 2, core: 2. Of those that a mesh axis runs over, the one named last changes fastest.
Arguments:
- x: bfloat16 [16, 4096, 1024], P(('rep', 'r', 's'))
- dy: bfloat16 [16, 4096, 1024], P(('rep', 'r', 's'))
- w_gate: bfloat16 [2, 1024, 2816], P(None, 's')
- w_up: bfloat16 [2, 1024, 2816], P(None, 's')
- w_down: bfloat16 [2, 2816, 1024], P(None, 's')
- m_w_gate: float32 [2, 1024, 2816], P(None, 's')
- m_w_up: float32 [2, 1024, 2816], P(None, 's')
- m_w_down: float32 [2, 2816, 1024], P(None, 's')
- v_w_gate: float32 [2, 1024, 2816], P(None, 's')
- v_w_up: float32 [2, 1024, 2816], P(None, 's')
- v_w_down: float32 [2, 2816, 1024], P(None, 's')
Outputs:
- output 1: bfloat16 [2, 1024, 2816], P('rep', 's')
- output 2: bfloat16 [2, 1024, 2816], P('rep', 's')
- output 3: bfloat16 [2, 2816, 1024], P('rep', 's')
- output 4: float32 [2, 1024, 2816], P('rep', 's')
- output 5: float32 [2, 1024, 2816], P('rep', 's')
- output 6: float32 [2, 2816, 1024], P('rep', 's')
- output 7: float32 [2, 1024, 2816], P('rep', 's')
- output 8: float32 [2, 1024, 2816], P('rep', 's')
- output 9: float32 [2, 2816, 1024], P('rep', 's')
All inputs are finite; a program needn't handle non-finite values.
Results may differ from the reference program's by a relative error of at most 0.02.
Values are sent between devices in bfloat16 or wider.
A program may use at most 2 GiB of HBM per device.

```python
import jax
import jax.numpy as jnp
from jax import lax

SEQUENCES = 16
TOKENS = 4096
D = 1024
FF = 2816
LAYERS = 2
NAMES = ("w_gate", "w_up", "w_down")
SHAPES = {"w_gate": (LAYERS, D, FF), "w_up": (LAYERS, D, FF), "w_down": (LAYERS, FF, D)}


def bump(key, n, height):
    away = (jnp.arange(n, dtype=jnp.int32) - jax.random.randint(key, (), 0, n, jnp.int32)) % n
    return jnp.where(away < n // 8, height, 1.0)


def together(key, own, strength):
    shared = jax.random.normal(key, own.shape[1:], jnp.float32)
    return (own + strength * shared) * lax.rsqrt(1 + strength * strength)


def setup_inputs(seed: int = 0, part: int = 0) -> dict:
    kx, kdy, ka, kb, kz, kf, kh, kl, *keys = jax.random.split(jax.random.key(seed), 8 + 3 * len(NAMES))
    kx, kdy, ka, kb = (jax.random.fold_in(k, part) for k in (kx, kdy, ka, kb))
    kw, km, kv = (keys[i::3] for i in range(3))
    shape = (SEQUENCES, TOKENS, D)
    much_x, much_dy = jax.random.uniform(kz, (2,), jnp.float32, 0.0, 1.0)
    loud = 2.0 ** jax.random.uniform(jax.random.fold_in(kz, 1), (), jnp.float32, -1.0, 2.0)
    layers = 2.0 ** jax.random.uniform(kl, (LAYERS, 1, 1), jnp.float32, -1.0, 1.0)
    x = together(ka, jax.random.normal(kx, shape, jnp.float32), much_x) * bump(kf, D, 4.0)
    dy = together(kb, jax.random.normal(kdy, shape, jnp.float32), much_dy)
    drawn = {"x": x.astype(jnp.bfloat16), "dy": (loud * dy * (SEQUENCES * TOKENS) ** -0.5).astype(jnp.bfloat16)}
    for key, name in zip(kw, NAMES, strict=True):
        w = jax.random.normal(key, SHAPES[name], jnp.float32) * SHAPES[name][1] ** -0.5
        drawn[name] = (w * {"w_gate": 1.0, "w_up": bump(kh, FF, 4.0), "w_down": layers}[name]).astype(jnp.bfloat16)
    for key, name in zip(km, NAMES, strict=True):
        drawn[f"m_{name}"] = 0.1 * jax.random.normal(key, SHAPES[name], jnp.float32)
    for key, name in zip(kv, NAMES, strict=True):
        drawn[f"v_{name}"] = jax.random.uniform(key, SHAPES[name], jnp.float32, 0.005, 0.015)
    return drawn


def matmul(a, w):
    return jnp.dot(a, w, preferred_element_type=jnp.float32).astype(jnp.bfloat16)


def normed(h):
    wide = h.astype(jnp.float32)
    scale = lax.rsqrt(jnp.mean(wide**2, -1, keepdims=True) + 1e-6)
    return (wide * scale).astype(jnp.bfloat16)


def layer(h, w):
    a = normed(h)
    gate = jnp.dot(a, w["w_gate"], preferred_element_type=jnp.float32)
    up = jnp.dot(a, w["w_up"], preferred_element_type=jnp.float32)
    return h + matmul((jax.nn.silu(gate) * up).astype(jnp.bfloat16), w["w_down"])


def adamw(w, m, v, g):
    m = 0.9 * m + 0.1 * g
    v = 0.95 * v + 0.05 * g * g
    step = m * lax.rsqrt(v + 1e-8) + 0.1 * w
    return (w - 0.02 * step).astype(jnp.bfloat16), m, v


def stack(weights, h):
    return lax.scan(lambda h, w: (layer(h, w), None), h, weights)[0]


def reference(x, dy, w_gate, w_up, w_down, m_w_gate, m_w_up, m_w_down, v_w_gate, v_w_up, v_w_down):
    weights = dict(zip(NAMES, (w_gate, w_up, w_down), strict=True))

    def take(so_far, sequence):
        h, by_y = sequence
        _, back = jax.vjp(lambda w: stack(w, h), weights)
        return jax.tree.map(lambda total, term: total + term.astype(jnp.float32), so_far, back(by_y)[0]), None

    none_yet = {name: jnp.zeros(w.shape, jnp.float32) for name, w in weights.items()}
    by_weights, _ = lax.scan(take, none_yet, (x, dy))
    gradients = [by_weights[name].astype(jnp.bfloat16).astype(jnp.float32) for name in NAMES]
    new = [
        adamw(w.astype(jnp.float32), m, v, g)
        for w, m, v, g in zip((w_gate, w_up, w_down), (m_w_gate, m_w_up, m_w_down), (v_w_gate, v_w_up, v_w_down), gradients, strict=True)
    ]
    return tuple(one[which] for which in range(3) for one in new)
```

```python
import functools

import jax
import jax.numpy as jnp
from jax import lax
from jax.experimental import pallas as pl
from jax.experimental.pallas import tpu as pltpu
from jax.sharding import PartitionSpec as P

BF, F32 = jnp.bfloat16, jnp.float32
VMEM_LIMIT = 62 * 1024 * 1024


def dot(a, b, ca=1, cb=0):
    return lax.dot_general(a, b, (((ca,), (cb,)), ((), ())), preferred_element_type=F32)


def chunks(width, size):
    return [(at, min(size, width - at)) for at in range(0, width, size)]


def load(owners, blocks, whole, sems, first):
    rows = blocks[0].shape[0]
    copies = []
    for i, block in enumerate(blocks):
        at = pl.multiple_of(owners[i] * rows, 16)
        copies.append(pltpu.make_async_copy(block, whole.at[pl.ds(at, rows), :], sems.at[first + i]))
    return copies


def normed(h):
    wide = h.astype(F32)
    scale = lax.rsqrt(jnp.mean(wide * wide, -1, keepdims=True) + 1e-6)
    return wide, scale


def k1_body(owners, h_ref, *refs):
    blocks, (at_ref, gate_ref, up_ref, hid_ref, hidt_ref, whole, sems) = refs[:8], refs[8:]

    @pl.when(pl.program_id(0) == 0)
    def _():
        copies = load(owners, blocks, whole, sems, 0)
        for copy in copies:
            copy.start()
        for copy in copies:
            copy.wait()

    wide, scale = normed(h_ref[...])
    a = (wide * scale).astype(BF)
    at_ref[...] = a.T
    ff = gate_ref.shape[1]
    for at, size in chunks(ff, 256):
        here = pl.ds(at, size)
        gate = dot(a, whole[:, here])
        up = dot(a, whole[:, pl.ds(ff + at, size)])
        gate_ref[:, here] = gate
        up_ref[:, here] = up
        hid = (gate * jax.nn.sigmoid(gate) * up).astype(BF)
        hid_ref[:, here] = hid
        hidt_ref[here, :] = hid.T


def k2_body(owners, x_ref, hid_ref, *refs):
    blocks, (h_ref, whole, sems) = refs[:8], refs[8:]

    @pl.when(pl.program_id(0) == 0)
    def _():
        copies = load(owners, blocks, whole, sems, 0)
        for copy in copies:
            copy.start()
        for copy in copies:
            copy.wait()

    for at, size in chunks(h_ref.shape[1], 512):
        here = pl.ds(at, size)
        out = dot(hid_ref[...], whole[:, here]).astype(BF)
        h_ref[:, here] = (x_ref[:, here].astype(F32) + out.astype(F32)).astype(BF)


def k3_body(owners, h_ref, dy_ref, *refs):
    gu, down, (at_ref, hidt_ref, dgu_ref, dh_ref, wgu, wd, dag, dau, sems) = refs[:8], refs[8:16], refs[16:]

    @pl.when(pl.program_id(0) == 0)
    def _():
        copies = load(owners, gu, wgu, sems, 0) + load(owners, down, wd, sems, 8)
        for copy in copies:
            copy.start()
        for copy in copies:
            copy.wait()

    wide, scale = normed(h_ref[...])
    a = (wide * scale).astype(BF)
    at_ref[...] = a.T
    dy = dy_ref[...]
    ff = hidt_ref.shape[0]
    for at, size in chunks(ff, 256):
        here, there = pl.ds(at, size), pl.ds(ff + at, size)
        gate = dot(a, wgu[:, here])
        up = dot(a, wgu[:, there])
        dhid = dot(dy, wd[here, :], 1, 1).astype(BF).astype(F32)
        s = jax.nn.sigmoid(gate)
        silu = gate * s
        hidt_ref[here, :] = (silu * up).astype(BF).T
        dup = (dhid * silu).astype(BF)
        dgate = (dhid * up * (s + silu * (1.0 - s))).astype(BF)
        dgu_ref[:, here] = dgate
        dgu_ref[:, there] = dup
    dag[...] = dot(dgu_ref[:, :ff], wgu[:, :ff], 1, 1).astype(BF)
    dau[...] = dot(dgu_ref[:, ff:], wgu[:, ff:], 1, 1).astype(BF)
    da = (dag[...].astype(F32) + dau[...].astype(F32)).astype(BF).astype(F32)
    wide = h_ref[...].astype(F32)
    inner = jnp.mean(da * wide, -1, keepdims=True)
    dwide = da * scale - wide * (inner * scale * scale * scale)
    dh_ref[...] = (dy.astype(F32) + dwide.astype(BF).astype(F32)).astype(BF)


def k4_body(owners, dh_ref, gate_ref, up_ref, *refs):
    down, (dgu_ref, wd, sems) = refs[:8], refs[8:]

    @pl.when(pl.program_id(0) == 0)
    def _():
        copies = load(owners, down, wd, sems, 0)
        for copy in copies:
            copy.start()
        for copy in copies:
            copy.wait()

    dh = dh_ref[...]
    ff = gate_ref.shape[1]
    for at, size in chunks(ff, 256):
        here, there = pl.ds(at, size), pl.ds(ff + at, size)
        dhid = dot(dh, wd[here, :], 1, 1).astype(BF).astype(F32)
        gate, up = gate_ref[:, here], up_ref[:, here]
        s = jax.nn.sigmoid(gate)
        silu = gate * s
        dgu_ref[:, there] = (dhid * silu).astype(BF)
        dgu_ref[:, here] = (dhid * up * (s + silu * (1.0 - s))).astype(BF)


def tokens_call(body, owners, tiled, blocks, outs, scratch, bm, flops, moved):
    t = tiled[0].shape[0]
    grid_spec = pltpu.PrefetchScalarGridSpec(
        num_scalar_prefetch=1,
        grid=(t // bm,),
        in_specs=[pl.BlockSpec((bm, v.shape[1]), lambda i, o: (i, 0)) for v in tiled] + [pl.BlockSpec(memory_space=pl.ANY)] * len(blocks),
        out_specs=[
            pl.BlockSpec((bm, shape[1]), lambda i, o: (i, 0)) if dim == 0 else pl.BlockSpec((shape[0], bm), lambda i, o: (0, i))
            for shape, _, dim in outs
        ],
        scratch_shapes=scratch + [pltpu.SemaphoreType.DMA((len(blocks),))],
    )
    return pl.pallas_call(
        body,
        grid_spec=grid_spec,
        out_shape=[jax.ShapeDtypeStruct(shape, dtype) for shape, dtype, _ in outs],
        compiler_params=pltpu.CompilerParams(dimension_semantics=("arbitrary",), vmem_limit_bytes=VMEM_LIMIT),
        cost_estimate=pl.CostEstimate(flops=flops, bytes_accessed=moved, transcendentals=0),
        name=body.__name__,
    )(owners, *tiled, *blocks)


def dw_body(added, split, order, lhs_ref, rhs_ref, *refs):
    add_ref = refs[0] if added else None
    outs, (lhs, sems) = refs[1 if added else 0 : -2], refs[-2:]
    rows = lhs.shape[0] // 4

    @pl.when(pl.program_id(0) == 0)
    def _():
        copies = []
        for i in range(4):
            at = pl.multiple_of(order[i] * rows, 16)
            copies.append(pltpu.make_async_copy(lhs_ref.at[pl.ds(at, rows), :], lhs.at[pl.ds(i * rows, rows), :], sems.at[i]))
        for copy in copies:
            copy.start()
        for copy in copies:
            copy.wait()

    total = dot(lhs[...], rhs_ref[...])
    if added:
        total = total + add_ref[...].astype(F32)
    if split:
        outs[0][...] = total[: 2 * rows].astype(BF)
        outs[1][...] = total[2 * rows :]
    else:
        outs[0][...] = total.astype(BF)


def dw(lhs, rhs, order, nb, add=None, first=0, width=None):
    rows, (t, _) = lhs.shape[0] // 8, rhs.shape
    width = width or rhs.shape[1]
    at = first // nb
    tall = pl.BlockSpec((4 * rows, nb), lambda n, o: (0, n))
    half = pl.BlockSpec((2 * rows, nb), lambda n, o: (0, n))
    if add is None:
        out_specs, out_shape = [tall], [jax.ShapeDtypeStruct((4 * rows, width), BF)]
    else:
        out_specs = [half, half]
        out_shape = [jax.ShapeDtypeStruct((2 * rows, width), BF), jax.ShapeDtypeStruct((2 * rows, width), F32)]
    grid_spec = pltpu.PrefetchScalarGridSpec(
        num_scalar_prefetch=1,
        grid=(width // nb,),
        in_specs=[pl.BlockSpec(memory_space=pl.ANY), pl.BlockSpec((t, nb), lambda n, o: (0, n + at))] + ([] if add is None else [tall]),
        out_specs=out_specs,
        scratch_shapes=[pltpu.VMEM((4 * rows, t), BF), pltpu.SemaphoreType.DMA((4,))],
    )
    out = pl.pallas_call(
        functools.partial(dw_body, add is not None, add is not None),
        grid_spec=grid_spec,
        out_shape=out_shape,
        compiler_params=pltpu.CompilerParams(dimension_semantics=("arbitrary",), vmem_limit_bytes=VMEM_LIMIT),
        cost_estimate=pl.CostEstimate(flops=8 * rows * t * width, bytes_accessed=2 * (4 * rows * t + t * width), transcendentals=0),
        name="dw_first" if add is None else "dw_second",
    )(order, lhs, rhs, *([] if add is None else [add]))
    return out[0] if add is None else out


def adam_body(n_prev, w_ref, m_ref, v_ref, own_ref, other_ref, *refs):
    new_w, new_m, new_v = refs[n_prev:]
    g = (own_ref[...].astype(F32) + other_ref[...].astype(F32)).astype(BF).astype(F32)
    m = 0.9 * m_ref[0] + 0.1 * g
    v = 0.95 * v_ref[0] + 0.05 * g * g
    w = w_ref[0].astype(F32)
    step = m * lax.rsqrt(v + 1e-8) + 0.1 * w
    new_w[0] = (w - 0.02 * step).astype(BF)
    new_m[0] = m
    new_v[0] = v


def adam(layer, w, m, v, own, other, cb, shift=0, prev=None):
    _, rows, columns = w.shape
    state = pl.BlockSpec((1, rows, cb), lambda j: (layer, 0, j))
    term = pl.BlockSpec((rows, cb), lambda j: (0, j + shift))
    prev = [] if prev is None else list(prev)
    return pl.pallas_call(
        functools.partial(adam_body, len(prev)),
        grid=(columns // cb,),
        in_specs=[state] * 3 + [term] * 2 + [pl.BlockSpec(memory_space=pl.ANY)] * len(prev),
        out_specs=[state] * 3,
        out_shape=[jax.ShapeDtypeStruct(w.shape, BF), jax.ShapeDtypeStruct(w.shape, F32), jax.ShapeDtypeStruct(w.shape, F32)],
        input_output_aliases={5 + i: i for i in range(len(prev))},
        compiler_params=pltpu.CompilerParams(dimension_semantics=("arbitrary",), vmem_limit_bytes=VMEM_LIMIT),
        cost_estimate=pl.CostEstimate(flops=20 * rows * columns, bytes_accessed=24 * rows * columns, transcendentals=0),
        name="adam",
    )(w, m, v, own, other, *prev)


def solution(mesh):
    assert mesh.shape["s"] == 8 and mesh.shape["r"] == 2, "mesh"
    both = ("r", "s")
    every = [(r, s) for r in range(2) for s in range(8)]

    def moved(value, flip):
        pairs = []
        for r, s in every:
            fr, fs = flip(r)
            pairs.append((r * 8 + s, (r ^ fr) * 8 + (s ^ fs)))
        return lax.ppermute(value, both, pairs)

    core = lambda v: moved(v, lambda r: (0, 1))
    over_x = lambda v: moved(v, lambda r: (0, 4))
    over_y = lambda v: moved(v, lambda r: (0, 2))
    over_z = lambda v: moved(v, lambda r: (1, 0))

    def gathered(block):
        one = moved(block, lambda r: (0, 2 if r else 4))
        two = moved(one, lambda r: (0, 4 if r else 2))
        three = over_z(one)
        mine = [block, one, two, three]
        return mine + [core(b) for b in mine]

    def step(x, dy, *arrays):
        (wg, wu, wd), m, v = (arrays[i : i + 3] for i in (0, 3, 6))
        x, dy = x[0], dy[0]
        t, d = x.shape
        ff = wg.shape[2]
        r, s = lax.axis_index("r"), lax.axis_index("s")
        near = jnp.where(r == 0, 4, 2)
        owners = jnp.stack([s, s ^ near, s ^ 6, s ^ (6 - near)])
        owners = jnp.concatenate([owners, owners ^ 1]).astype(jnp.int32)
        by_x = jnp.stack([s ^ 6, s ^ 4, s ^ 2, s]).astype(jnp.int32)
        by_y = jnp.stack([s ^ 6, s ^ 2, s ^ 4, s]).astype(jnp.int32)

        gu0 = gathered(jnp.concatenate([wg[0], wu[0]], 1))
        d0 = gathered(wd[0])
        gu1 = gathered(jnp.concatenate([wg[1], wu[1]], 1))
        d1 = gathered(wd[1])

        one = 2 * t * d * ff
        bm = 256
        at0, gate, up, hid, hidt0 = tokens_call(
            k1_body, owners, [x], gu0,
            [((d, t), BF, 1), ((t, ff), F32, 0), ((t, ff), F32, 0), ((t, ff), BF, 0), ((ff, t), BF, 1)],
            [pltpu.VMEM((d, 2 * ff), BF)], bm, 2 * one, 12 * t * ff,
        )
        (h1,) = tokens_call(k2_body, owners, [x, hid], d0, [((t, d), BF, 0)], [pltpu.VMEM((ff, d), BF)], 512, one, 2 * t * ff)
        at1, hidt1, dgu1, dh1 = tokens_call(
            k3_body, owners, [h1, dy], gu1 + d1,
            [((d, t), BF, 1), ((ff, t), BF, 1), ((t, 2 * ff), BF, 0), ((t, d), BF, 0)],
            [pltpu.VMEM((d, 2 * ff), BF), pltpu.VMEM((ff, d), BF), pltpu.VMEM((bm, d), BF), pltpu.VMEM((bm, d), BF)], bm, 5 * one, 6 * t * ff,
        )

        def reduced(send, keep, x_first):
            first, second = (over_x, over_y) if x_first else (over_y, over_x)
            rows = send.shape[0] // 2
            got = keep + first(send).astype(F32)
            own = (got[rows:] + second(got[:rows].astype(BF)).astype(F32)).astype(BF)
            return own, over_z(own)

        dgu1_a = core(dw(at1, dgu1, by_x ^ 1, 512))
        dd1_a = core(dw(hidt1, dy, by_y ^ 1, 256))
        gu1_sum = reduced(*dw(at1, dgu1, by_x, 512, dgu1_a), True)
        d1_sum = reduced(*dw(hidt1, dy, by_y, 256, dd1_a), False)
        dd0_a = core(dw(hidt0, dh1, by_x ^ 1, 256))
        (dgu0,) = tokens_call(k4_body, owners, [dh1, gate, up], d0, [((t, 2 * ff), BF, 0)], [pltpu.VMEM((ff, d), BF)], bm, one, 12 * t * ff)
        dg0_a = core(dw(at0, dgu0, by_y ^ 1, 256, first=0, width=ff))
        d0_sum = reduced(*dw(hidt0, dh1, by_x, 256, dd0_a), True)
        du0_a = core(dw(at0, dgu0, by_x ^ 1, 256, first=ff, width=ff))
        g0_sum = reduced(*dw(at0, dgu0, by_y, 256, dg0_a, 0, ff), False)
        u0_sum = reduced(*dw(at0, dgu0, by_x, 256, du0_a, ff, ff), True)

        new_g = adam(1, wg, m[0], v[0], *gu1_sum, 1408)
        new_u = adam(1, wu, m[1], v[1], *gu1_sum, 1408, 2)
        new_d = adam(1, wd, m[2], v[2], *d1_sum, 512)
        new_d = adam(0, wd, m[2], v[2], *d0_sum, 512, 0, new_d)
        new_g = adam(0, wg, m[0], v[0], *g0_sum, 1408, 0, new_g)
        new_u = adam(0, wu, m[1], v[1], *u0_sum, 1408, 0, new_u)
        return tuple(new[which] for which in range(3) for new in (new_g, new_u, new_d))

    states, cut = P(("rep", "r", "s"), None, None), P(None, "s", None)
    return jax.shard_map(
        step,
        mesh=mesh,
        in_specs=(states, states) + (cut,) * 9,
        out_specs=(P("rep", "s", None),) * 9,
        check_vma=False,
    )
```
